32 devices in a mesh: fields: 1 (over z), col: 4 (over y), row: 8 (over x, core).
Axes of the slice: x: 4, y: 4, z: 1, core: 2. Of those that a mesh axis runs over, the one named last changes fastest.
The devices are a block of a 4x4x8 slice.
Arguments:
- field_u: bfloat16 [32, 128, 128, 128], P('fields', None, 'row', 'col')
- fac_a: bfloat16 [128, 128], P('fields')
- fac_b: bfloat16 [128, 128], P('fields')
- fac_c: bfloat16 [128, 128], P('fields')
- diag_d: float32 [128, 128, 128], P(('fields', 'row'), 'col')
Outputs:
- output: float32 [32, 128, 128, 128], P('fields', None, 'row', 'col')
All inputs are finite; a program needn't handle non-finite values.
Results may differ from the reference program's by a relative error of at most 0.00108.
Values are sent between devices in bfloat16 or wider.
A program may use at most 768 MiB of HBM per device.

```python
import jax
import jax.numpy as jnp
from jax import lax

N = 128
BATCH = 32


def setup_inputs(seed: int = 0, part: int = 0) -> dict:
    base_key = jax.random.fold_in(jax.random.key(seed), part)
    key_field, key_a, key_b, key_c, key_diag = jax.random.split(base_key, 5)
    fan_scale = N ** -0.5
    field_u = jax.random.normal(key_field, (BATCH, N, N, N), jnp.float32)
    fac_a = jax.random.normal(key_a, (N, N), jnp.float32) * fan_scale
    fac_b = jax.random.normal(key_b, (N, N), jnp.float32) * fan_scale
    fac_c = jax.random.normal(key_c, (N, N), jnp.float32) * fan_scale
    diag_d = jnp.exp(0.5 * jax.random.normal(key_diag, (N, N, N), jnp.float32))
    return {"field_u": field_u.astype(jnp.bfloat16), "fac_a": fac_a.astype(jnp.bfloat16), "fac_b": fac_b.astype(jnp.bfloat16), "fac_c": fac_c.astype(jnp.bfloat16), "diag_d": diag_d}


def reference(field_u, fac_a, fac_b, fac_c, diag_d):
    mat_a = fac_a.astype(jnp.float32)
    mat_b = fac_b.astype(jnp.float32)
    mat_c = fac_c.astype(jnp.float32)
    scales = diag_d.astype(jnp.float32)

    def to_bf16(values_in):
        return values_in.astype(jnp.bfloat16).astype(jnp.float32)

    def one_tensor(tensor):
        stage_one = to_bf16(jnp.einsum("ix,xyz->iyz", mat_a, tensor.astype(jnp.float32)))
        stage_two = to_bf16(jnp.einsum("jy,iyz->ijz", mat_b, stage_one))
        stage_three = to_bf16(jnp.einsum("kz,ijz->ijk", mat_c, stage_two) * scales)
        stage_four = to_bf16(jnp.einsum("kz,ijk->ijz", mat_c, stage_three))
        stage_five = to_bf16(jnp.einsum("jy,ijz->iyz", mat_b, stage_four))
        return jnp.einsum("ix,iyz->xyz", mat_a, stage_five)

    return lax.map(one_tensor, field_u)
```

```python
import functools

import jax
import jax.numpy as jnp
from jax import lax
from jax.experimental import pallas as pl
from jax.experimental.pallas import tpu as pltpu
from jax.sharding import PartitionSpec as P

MESH = pl.DeviceIdType.MESH
F32, BF16 = jnp.float32, jnp.bfloat16
CORES = 2
QUAD = 4
HALF = 16
LANES = 128
PITCH_A = 24
PITCH_B = 40


def fill_spread(a_ref, w_ref, slabs):
    n = a_ref.shape[0]
    slab = n // slabs
    w_ref[...] = jnp.zeros_like(w_ref)
    for s in range(slabs):
        for b in range(QUAD):
            w_ref[pl.ds(s * n + b * slab, slab), pl.ds(b * n, n)] = a_ref[pl.ds(s * slab, slab), :]


def exchange_kernel(n_row, n_col, u_hbm, a_ref, b_ref, c_ref, d_hbm, out_hbm,
                    u_v, w_v, bt_v, ct_v, d_v, dt_v, scr_a, scr_b, scr_c,
                    send_f, recv_f, send_cf, recv_cf, send_cb, recv_cb, send_b,
                    u_sem, d_sem, d_send, d_recv, own_sem, sf, rf, scf, rcf, scb, rcb, sb, rb):
    me = lax.axis_index("row")
    mc = lax.axis_index("col")
    slabs = n_row // CORES
    n = a_ref.shape[0]
    chunks = u_v.shape[0] // (CORES * QUAD)
    yl, zl = u_v.shape[1], u_v.shape[2]
    halves = zl // HALF
    units = chunks * halves
    jl = n // n_col
    il = d_v.shape[0] // CORES
    group = CORES * QUAD

    def load_u(q, h):
        sl = (pl.ds(q * group, group), slice(None), pl.ds(h * HALF, HALF))
        return pltpu.make_async_copy(u_hbm.at[sl], u_v.at[sl], u_sem.at[q * halves + h])

    for q in range(chunks):
        for h in range(halves):
            load_u(q, h).start()
    core = lax.rem(me, CORES)
    own_d = pltpu.make_async_copy(d_hbm, d_v.at[pl.ds(core * il, il)], d_sem)
    own_d.start()

    barrier = pltpu.get_barrier_semaphore()
    for k in range(1, n_row):
        pl.semaphore_signal(barrier, inc=1, device_id={"row": lax.rem(me + k, n_row)}, device_id_type=MESH)
    for k in range(1, n_col):
        pl.semaphore_signal(barrier, inc=1, device_id={"col": lax.rem(mc + k, n_col)}, device_id_type=MESH)

    fill_spread(a_ref, w_v, slabs)
    bt_v[...] = b_ref[...].astype(F32).T.astype(BF16)
    ct_v[...] = c_ref[...].astype(F32).T.astype(BF16)

    pl.semaphore_wait(barrier, n_row + n_col - 2)

    partner = me + 1 - 2 * core
    pair_d = pltpu.make_async_remote_copy(
        d_hbm, d_v.at[pl.ds(core * il, il)], d_send, d_recv, device_id={"row": partner}, device_id_type=MESH)
    pair_d.start()

    def stage_one(t):
        q, h = t // halves, lax.rem(t, halves)
        zs = pl.ds(pl.multiple_of(h * HALF, HALF), HALF)
        load_u(q, h).wait()
        for g in range(CORES):
            lhs = jnp.concatenate(
                [u_v[q * group + g * QUAD + b, :, zs, :].reshape(yl * HALF, n) for b in range(QUAD)], axis=1)
            out = lax.dot_general(lhs, w_v[...], (((1,), (1,)), ((), ())), preferred_element_type=F32)
            for s in range(slabs):
                for y in range(yl):
                    scr_a[s, pl.ds(y, HALF, stride=PITCH_A), :] = out[y * HALF:(y + 1) * HALF, s * LANES:(s + 1) * LANES]
            for s in range(slabs):
                rows = scr_a[s].reshape(HALF, PITCH_A, LANES)[:, :yl, :]
                send_f[q, s * CORES + g, zs] = rows.astype(BF16)
        mine = pl.ds(pl.multiple_of(me * yl, yl), yl)
        recv_f[q, zs, mine, :] = send_f[q, me, zs]
        for k in range(1, n_row):
            to = lax.rem(me + k, n_row)
            pltpu.make_async_remote_copy(
                send_f.at[q, to, zs], recv_f.at[q, zs, mine, :], sf, rf.at[t],
                device_id={"row": to}, device_id_type=MESH).start()

    def stage_two(t):
        q, h = t // halves, lax.rem(t, halves)
        zs = pl.ds(pl.multiple_of(h * HALF, HALF), HALF)
        got = recv_f.at[q, zs, pl.ds(0, n - yl), :]
        pltpu.make_async_copy(got, got, rf.at[t]).wait()

        def some(i, _):
            for p in range(4):
                z = h * HALF + i * 8 + p * 2
                rhs = jnp.concatenate([recv_f[q, z], recv_f[q, z + 1]], axis=1)
                out = jnp.dot(b_ref[...], rhs, preferred_element_type=F32)
                for e in range(2):
                    scr_b[pl.ds(i * 8 + p * 2 + e, n, stride=PITCH_A), :] = out[:, e * LANES:(e + 1) * LANES]
            return 0

        lax.fori_loop(0, HALF // 8, some, 0)
        for c in range(n_col):
            rows = scr_b[pl.ds(c * jl * PITCH_A, jl * PITCH_A), :].reshape(jl, PITCH_A, LANES)[:, :HALF, :]
            send_cf[q, h, c] = rows.astype(BF16)
        mine = pl.ds(pl.multiple_of(mc * zl + h * HALF, HALF), HALF)
        recv_cf[q, :, mine, :] = send_cf[q, h, mc]
        for k in range(1, n_col):
            to = lax.rem(mc + k, n_col)
            pltpu.make_async_remote_copy(
                send_cf.at[q, h, to], recv_cf.at[q, :, mine, :], scf, rcf.at[t],
                device_id={"col": to}, device_id_type=MESH).start()

    def stage_mid(q, part):
        @pl.when(part == 0)
        def _():
            for h in range(halves):
                got = recv_cf.at[q, :, pl.ds(0, (n_col - 1) * HALF), :]
                pltpu.make_async_copy(got, got, rcf.at[q * halves + h]).wait()

        def some(i, _):
            for p in range(4):
                j = part * (jl // 2) + i * 8 + p * 2
                rhs = jnp.concatenate([recv_cf[q, j], recv_cf[q, j + 1]], axis=1)
                mid = jnp.dot(c_ref[...], rhs, preferred_element_type=F32)
                mid = (mid * jnp.concatenate([dt_v[j], dt_v[j + 1]], axis=1)).astype(BF16)
                out = jnp.dot(ct_v[...], mid, preferred_element_type=F32)
                for e in range(2):
                    scr_c[pl.ds(j + e, n, stride=PITCH_B), :] = out[:, e * LANES:(e + 1) * LANES]
            return 0

        lax.fori_loop(0, jl // 16, some, 0)

        @pl.when(part == 1)
        def _():
            for h in range(halves):
                for c in range(n_col):
                    rows = scr_c[pl.ds((c * zl + h * HALF) * PITCH_B, HALF * PITCH_B), :]
                    send_cb[q, h, c] = rows.reshape(HALF, PITCH_B, LANES)[:, :jl, :].astype(BF16)
                zs = pl.ds(h * HALF, HALF)
                mine = pl.ds(pl.multiple_of(mc * jl, jl), jl)
                recv_cb[q, zs, mine, :] = send_cb[q, h, mc]
                for k in range(1, n_col):
                    to = lax.rem(mc + k, n_col)
                    pltpu.make_async_remote_copy(
                        send_cb.at[q, h, to], recv_cb.at[q, zs, mine, :], scb, rcb.at[q * halves + h],
                        device_id={"col": to}, device_id_type=MESH).start()

    def stage_five(t):
        q, h = t // halves, lax.rem(t, halves)
        zs = pl.ds(pl.multiple_of(h * HALF, HALF), HALF)
        got = recv_cb.at[q, zs, pl.ds(0, n - jl), :]
        pltpu.make_async_copy(got, got, rcb.at[t]).wait()

        def some(i, _):
            for p in range(4):
                z = h * HALF + i * 8 + p * 2
                rhs = jnp.concatenate([recv_cb[q, z], recv_cb[q, z + 1]], axis=1)
                out = jnp.dot(bt_v[...], rhs, preferred_element_type=F32)
                for e in range(2):
                    scr_b[pl.ds(i * 8 + p * 2 + e, n, stride=PITCH_A), :] = out[:, e * LANES:(e + 1) * LANES]
            return 0

        lax.fori_loop(0, HALF // 8, some, 0)
        for r in range(n_row):
            rows = scr_b[pl.ds(r * yl * PITCH_A, yl * PITCH_A), :].reshape(yl, PITCH_A, LANES)[:, :HALF, :]
            send_b[q, h, r] = rows.astype(BF16)
        land = out_hbm.at[q, me, :, zs, :]
        for k in range(1, n_row):
            to = lax.rem(me + k, n_row)
            pltpu.make_async_remote_copy(
                send_b.at[q, h, to], land, sb, rb, device_id={"row": to}, device_id_type=MESH).start()
        pltpu.make_async_copy(send_b.at[q, h, me], land, own_sem).start()

    def build_d():
        own_d.wait()
        pair_d.wait()
        for j in range(jl):
            rows = d_v[:, j, :]
            dt_v[j] = jnp.concatenate([rows] * QUAD, axis=0).T

    last = units + 6

    def tick(t, _):
        @pl.when(t < units)
        def _():
            stage_one(t)

        @pl.when(t == 1)
        def _():
            build_d()

        @pl.when((t >= 2) & (t < units + 2))
        def _():
            stage_two(t - 2)

        @pl.when((t >= 5) & (t < units + 5))
        def _():
            stage_mid((t - 5) // halves, lax.rem(t - 5, halves))

        @pl.when(t >= 8)
        def _():
            stage_five(t - 8)

        return 0

    lax.fori_loop(0, units + 8, tick, 0)

    def drain(ref, sem):
        pltpu.make_async_copy(ref, ref, sem).wait()

    drain(send_f.at[:, pl.ds(0, n_row - 1)], sf)
    drain(send_cf.at[:, :, pl.ds(0, n_col - 1)], scf)
    drain(send_cb.at[:, :, pl.ds(0, n_col - 1)], scb)
    drain(send_b.at[:, :, pl.ds(0, n_row - 1)], sb)
    drain(send_b.at[:, :, 0], own_sem)
    drain(send_b.at[:, :, pl.ds(0, n_row - 1)], rb)


def last_kernel(slabs, a_ref, h_ref, w_ref, w_v):
    @pl.when(pl.program_id(0) == 0)
    def _():
        fill_spread(a_ref, w_v, slabs)

    yl, zl = h_ref.shape[3], h_ref.shape[4]
    lhs = jnp.concatenate([h_ref[0, s, 0].reshape(yl * zl, LANES) for s in range(slabs)], axis=1)
    out = jnp.dot(lhs, w_v[...], preferred_element_type=F32)
    for b in range(QUAD):
        w_ref[b] = out[:, b * LANES:(b + 1) * LANES].reshape(yl, zl, LANES)


def solution(mesh):
    spec_field = P("fields", None, "row", "col")
    spec_factor = P("fields", None)
    spec_diag = P(("fields", "row"), "col", None)
    n_row, n_col = mesh.shape["row"], mesh.shape["col"]
    slabs = n_row // CORES

    def local_apply(field_u, fac_a, fac_b, fac_c, diag_d):
        nb, n, yl, zl = field_u.shape
        il, jl, _ = diag_d.shape
        group = CORES * QUAD
        chunks = nb // group
        halves = zl // HALF
        units = chunks * halves
        u = jnp.transpose(field_u, (0, 2, 3, 1))
        vm = pl.BlockSpec(memory_space=pltpu.VMEM)
        hb = pl.BlockSpec(memory_space=pl.ANY)
        dma = pltpu.SemaphoreType.DMA
        moved = pl.pallas_call(
            functools.partial(exchange_kernel, n_row, n_col),
            out_shape=jax.ShapeDtypeStruct((chunks, n_row, yl, zl, LANES), BF16),
            in_specs=[hb, vm, vm, vm, hb],
            out_specs=hb,
            scratch_shapes=[
                pltpu.VMEM((nb, yl, zl, n), BF16),
                pltpu.VMEM((QUAD * n, QUAD * n), BF16),
                pltpu.VMEM((n, n), BF16),
                pltpu.VMEM((n, n), BF16),
                pltpu.VMEM((CORES * il, jl, n), F32),
                pltpu.VMEM((jl, n, LANES), F32),
                pltpu.VMEM((slabs, HALF * PITCH_A, LANES), F32),
                pltpu.VMEM((n * PITCH_A, LANES), F32),
                pltpu.VMEM((n * PITCH_B, LANES), F32),
                pltpu.VMEM((chunks, n_row, zl, yl, LANES), BF16),
                pltpu.VMEM((chunks, zl, n, LANES), BF16),
                pltpu.VMEM((chunks, halves, n_col, jl, HALF, LANES), BF16),
                pltpu.VMEM((chunks, jl, n, LANES), BF16),
                pltpu.VMEM((chunks, halves, n_col, HALF, jl, LANES), BF16),
                pltpu.VMEM((chunks, zl, n, LANES), BF16),
                pltpu.VMEM((chunks, halves, n_row, yl, HALF, LANES), BF16),
                dma((units,)), dma, dma, dma, dma,
                dma, dma((units,)), dma, dma((units,)), dma, dma((units,)), dma, dma,
            ],
            compiler_params=pltpu.CompilerParams(
                collective_id=0, has_side_effects=True, vmem_limit_bytes=60 * 2**20),
            name="pencils",
        )(u, fac_a, fac_b, fac_c, diag_d)
        moved = moved.reshape(chunks, slabs, CORES, yl, zl, LANES)
        w = pl.pallas_call(
            functools.partial(last_kernel, slabs),
            grid=(chunks * CORES,),
            out_shape=jax.ShapeDtypeStruct((nb, yl, zl, n), F32),
            in_specs=[
                pl.BlockSpec((n, n), lambda i: (0, 0)),
                pl.BlockSpec((1, slabs, 1, yl, zl, LANES), lambda i: (i // CORES, 0, i % CORES, 0, 0, 0)),
            ],
            out_specs=pl.BlockSpec((QUAD, yl, zl, n), lambda i: (i, 0, 0, 0)),
            scratch_shapes=[pltpu.VMEM((QUAD * n, QUAD * n), BF16)],
            name="last",
        )(fac_a, moved)
        return jnp.transpose(w, (0, 3, 1, 2))

    return jax.shard_map(local_apply, mesh=mesh, in_specs=(spec_field, spec_factor, spec_factor, spec_factor, spec_diag), out_specs=spec_field, check_vma=False)
```

```python
import functools

import jax
import jax.numpy as jnp
from jax import lax
from jax.experimental import pallas as pl
from jax.experimental.pallas import tpu as pltpu
from jax.sharding import PartitionSpec as P

MESH = pl.DeviceIdType.MESH
F32, BF16 = jnp.float32, jnp.bfloat16
CORES = 2
QUAD = 4
TILE = 16
UNIT = 8
LANES = 128
PITCH_Y = 24
PITCH_Z = 136
PITCH_J = 40


def fill_spread(a_ref, w_ref, slabs):
    n = a_ref.shape[0]
    slab = n // slabs
    w_ref[...] = jnp.zeros_like(w_ref)
    for s in range(slabs):
        for b in range(QUAD):
            w_ref[pl.ds(s * n + b * slab, slab), pl.ds(b * n, n)] = a_ref[pl.ds(s * slab, slab), :]


def exchange_kernel(n_row, n_col, u_hbm, a_hbm, b_hbm, c_hbm, d_hbm, w_ref,
                    u_v, a_ref, b_ref, c_ref, w_v, bt_v, ct_v, d_v, dt_v, scr_y, scr_z, scr_j,
                    send_f, recv_f, send_cf, recv_cf, send_cb, recv_cb, send_b, recv_b,
                    u_sem, abc_sem, d_sem, d_send, d_recv, sf, rf, scf, rcf, scb, rcb, sb, rb):
    me = lax.axis_index("row")
    mc = lax.axis_index("col")
    slabs = n_row // CORES
    n = a_ref.shape[0]
    group = CORES * QUAD
    chunks = u_v.shape[0] // group
    yl, zl = u_v.shape[1], u_v.shape[2]
    jl = n // n_col
    il = d_v.shape[0] // CORES
    tiles = zl // TILE
    per_tile = TILE // UNIT
    per_chunk = zl // UNIT
    units = chunks * per_chunk

    def load_u(q, p):
        sl = (pl.ds(q * group, group), slice(None), pl.ds(p * TILE, TILE))
        return pltpu.make_async_copy(u_hbm.at[sl], u_v.at[sl], u_sem.at[q * tiles + p])

    barrier = pltpu.get_barrier_semaphore()
    for k in range(1, n_row):
        pl.semaphore_signal(barrier, inc=1, device_id={"row": lax.rem(me + k, n_row)}, device_id_type=MESH)
    for k in range(1, n_col):
        pl.semaphore_signal(barrier, inc=1, device_id={"col": lax.rem(mc + k, n_col)}, device_id_type=MESH)

    factors = [pltpu.make_async_copy(x, v, abc_sem.at[k])
               for k, (x, v) in enumerate(((a_hbm, a_ref), (b_hbm, b_ref), (c_hbm, c_ref)))]
    factors[0].start()
    for q in range(chunks):
        for p in range(tiles):
            load_u(q, p).start()
    factors[1].start()
    factors[2].start()
    core = lax.rem(me, CORES)
    own_d = pltpu.make_async_copy(d_hbm, d_v.at[pl.ds(core * il, il)], d_sem)
    own_d.start()

    factors[0].wait()
    fill_spread(a_ref, w_v, slabs)

    partner = me + 1 - 2 * core
    pair_d = pltpu.make_async_remote_copy(
        d_hbm, d_v.at[pl.ds(core * il, il)], d_send, d_recv, device_id={"row": partner}, device_id_type=MESH)

    my_y = pl.ds(pl.multiple_of(me * yl, yl), yl)
    my_j = pl.ds(pl.multiple_of(mc * jl, jl), jl)

    def arrived(ref, sem):
        pltpu.make_async_copy(ref, ref, sem).wait()

    def stage_one(v):
        q, p = v // tiles, lax.rem(v, tiles)
        zs = pl.ds(pl.multiple_of(p * TILE, TILE), TILE)
        load_u(q, p).wait()
        for g in range(CORES):
            lhs = jnp.concatenate(
                [u_v[q * group + g * QUAD + b, :, zs, :].reshape(yl * TILE, n) for b in range(QUAD)], axis=1)
            out = lax.dot_general(lhs, w_v[...], (((1,), (1,)), ((), ())), preferred_element_type=F32)
            for s in range(slabs):
                for y in range(yl):
                    scr_y[s, pl.ds(y, TILE, stride=PITCH_Y), :] = out[y * TILE:(y + 1) * TILE, s * LANES:(s + 1) * LANES]
            for s in range(slabs):
                rows = scr_y[s].reshape(TILE, PITCH_Y, LANES)[:, :yl, :]
                send_f[q, s * CORES + g, zs] = rows.astype(BF16)
        recv_f[q, zs, my_y, :] = send_f[q, me, zs]

    def send_one(v):
        q, p = v // tiles, lax.rem(v, tiles)
        for e in range(per_tile):
            part = pl.ds(p * TILE + e * UNIT, UNIT)
            for k in range(1, n_row):
                to = lax.rem(me + k, n_row)
                pltpu.make_async_remote_copy(
                    send_f.at[q, to, part], recv_f.at[q, part, my_y, :], sf, rf.at[v * per_tile + e],
                    device_id={"row": to}, device_id_type=MESH).start()

    def stage_two(t):
        q, z0 = t // per_chunk, lax.rem(t, per_chunk) * UNIT
        zs = pl.ds(z0, UNIT)
        arrived(recv_f.at[q, zs, pl.ds(0, n - yl), :], rf.at[t])
        for p in range(0, UNIT, 2):
            rhs = jnp.concatenate([recv_f[q, z0 + p], recv_f[q, z0 + p + 1]], axis=1)
            out = jnp.dot(b_ref[...], rhs, preferred_element_type=F32).astype(BF16)
            for e in range(2):
                for c in range(n_col):
                    send_cf[q, c, z0 + p + e] = out[c * jl:(c + 1) * jl, e * LANES:(e + 1) * LANES]
        land = pl.ds(mc * zl + z0, UNIT)
        recv_cf[q, land] = send_cf[q, mc, zs]
        for k in range(1, n_col):
            to = lax.rem(mc + k, n_col)
            pltpu.make_async_remote_copy(
                send_cf.at[q, to, zs], recv_cf.at[q, land], scf, rcf.at[t],
                device_id={"col": to}, device_id_type=MESH).start()

    def collect(t):
        q, z0 = t // per_chunk, lax.rem(t, per_chunk) * UNIT
        arrived(recv_cf.at[q, pl.ds(0, (n_col - 1) * UNIT)], rcf.at[t])
        for c in range(n_col):
            for e in range(UNIT):
                z = c * zl + z0 + e
                scr_z[pl.ds(z, jl, stride=PITCH_Z), :] = recv_cf[q, z].astype(F32)

    def stage_mid(q):
        def some(i, _):
            for p in range(4):
                j = i * 8 + p * 2
                rhs = jnp.concatenate(
                    [scr_z[pl.ds(pl.multiple_of((j + e) * PITCH_Z, 8), n), :].astype(BF16) for e in range(2)], axis=1)
                mid = jnp.dot(c_ref[...], rhs, preferred_element_type=F32)
                mid = (mid * jnp.concatenate([dt_v[j], dt_v[j + 1]], axis=1)).astype(BF16)
                out = jnp.dot(ct_v[...], mid, preferred_element_type=F32)
                for e in range(2):
                    scr_j[pl.ds(j + e, n, stride=PITCH_J), :] = out[:, e * LANES:(e + 1) * LANES]
            return 0

        lax.fori_loop(0, jl // 8, some, 0)
        for c in range(n_col):
            rows = scr_j[pl.ds(c * zl * PITCH_J, zl * PITCH_J), :].reshape(zl, PITCH_J, LANES)[:, :jl, :]
            send_cb[q, c] = rows.astype(BF16)
        recv_cb[q, :, my_j, :] = send_cb[q, mc]

        def send(e, _):
            zs = pl.ds(e * UNIT, UNIT)
            for k in range(1, n_col):
                to = lax.rem(mc + k, n_col)
                pltpu.make_async_remote_copy(
                    send_cb.at[q, to, zs], recv_cb.at[q, zs, my_j, :], scb, rcb.at[q * per_chunk + e],
                    device_id={"col": to}, device_id_type=MESH).start()
            return 0

        lax.fori_loop(0, per_chunk, send, 0)

    def stage_five(t):
        q, z0 = t // per_chunk, lax.rem(t, per_chunk) * UNIT
        zs = pl.ds(z0, UNIT)
        arrived(recv_cb.at[q, zs, pl.ds(0, n - jl), :], rcb.at[t])
        for p in range(0, UNIT, 2):
            rhs = jnp.concatenate([recv_cb[q, z0 + p], recv_cb[q, z0 + p + 1]], axis=1)
            out = jnp.dot(bt_v[...], rhs, preferred_element_type=F32).astype(BF16)
            for e in range(2):
                for r in range(n_row):
                    send_b[q, r, z0 + p + e] = out[r * yl:(r + 1) * yl, e * LANES:(e + 1) * LANES]
        recv_b[q, me, zs] = send_b[q, me, zs]
        for k in range(1, n_row):
            to = lax.rem(me + k, n_row)
            pltpu.make_async_remote_copy(
                send_b.at[q, to, zs], recv_b.at[q, me, zs], sb, rb.at[t], device_id={"row": to}, device_id_type=MESH).start()

    def stage_six(t):
        q, z0 = t // per_chunk, lax.rem(t, per_chunk) * UNIT
        zs = pl.ds(z0, UNIT)
        arrived(recv_b.at[q, pl.ds(0, n_row - 1), zs], rb.at[t])
        for g in range(CORES):
            lhs = jnp.concatenate(
                [recv_b[q, s * CORES + g, zs].reshape(UNIT * yl, LANES) for s in range(slabs)], axis=1)
            out = jnp.dot(lhs, w_v[...], preferred_element_type=F32)
            for b in range(QUAD):
                for e in range(UNIT):
                    w_ref[q * group + g * QUAD + b, pl.ds(z0 + e, yl, stride=zl), :] = (
                        out[e * yl:(e + 1) * yl, b * LANES:(b + 1) * LANES])

    def build_d():
        own_d.wait()
        pair_d.wait()
        for j in range(jl):
            rows = d_v[:, j, :]
            dt_v[j] = jnp.concatenate([rows] * QUAD, axis=0).T

    stage_one(0)
    pl.semaphore_wait(barrier, n_row + n_col - 2)
    send_one(0)
    pair_d.start()
    stage_one(1)
    send_one(1)
    factors[1].wait()
    factors[2].wait()
    bt_v[...] = b_ref[...].astype(F32).T.astype(BF16)
    ct_v[...] = c_ref[...].astype(F32).T.astype(BF16)
    lead = 2
    lag = per_chunk
    after = lag + per_chunk + 1

    def tick(t, _):
        @pl.when(t < units)
        def _():
            stage_two(t)

        @pl.when((lax.rem(t, per_tile) == 0) & (t // per_tile + lead < chunks * tiles))
        def _():
            stage_one(t // per_tile + lead)
            send_one(t // per_tile + lead)

        @pl.when(t == 1)
        def _():
            build_d()

        @pl.when((t >= lag) & (t < units + lag))
        def _():
            collect(t - lag)

            @pl.when(lax.rem(t - lag, per_chunk) == per_chunk - 1)
            def _():
                stage_mid((t - lag) // per_chunk)

        @pl.when((t >= after) & (t < units + after))
        def _():
            stage_five(t - after)

        @pl.when(t >= after + 2)
        def _():
            stage_six(t - after - 2)

        return 0

    lax.fori_loop(0, units + after + 2, tick, 0)

    arrived(send_f.at[:, pl.ds(0, n_row - 1)], sf)
    arrived(send_cf.at[:, pl.ds(0, n_col - 1)], scf)
    arrived(send_cb.at[:, pl.ds(0, n_col - 1)], scb)
    arrived(send_b.at[:, pl.ds(0, n_row - 1)], sb)


def last_kernel(w_ref, w_hbm, sem):
    pieces = 8
    rows = w_ref.shape[0] // pieces
    for i in range(pieces):
        part = pl.ds(i * rows, rows)
        pltpu.make_async_copy(w_ref.at[part], w_hbm.at[part], sem).start()
    pltpu.make_async_copy(w_ref, w_hbm, sem).wait()


def solution(mesh):
    spec_field = P("fields", None, "row", "col")
    spec_factor = P("fields", None)
    spec_diag = P(("fields", "row"), "col", None)
    n_row, n_col = mesh.shape["row"], mesh.shape["col"]
    slabs = n_row // CORES

    def local_apply(field_u, fac_a, fac_b, fac_c, diag_d):
        nb, n, yl, zl = field_u.shape
        il, jl, _ = diag_d.shape
        chunks = nb // (CORES * QUAD)
        tiles = chunks * zl // TILE
        units = chunks * zl // UNIT
        u = jnp.transpose(field_u, (0, 2, 3, 1))
        vm = pl.BlockSpec(memory_space=pltpu.VMEM)
        hb = pl.BlockSpec(memory_space=pltpu.HBM)
        dma = pltpu.SemaphoreType.DMA
        done = pl.pallas_call(
            functools.partial(exchange_kernel, n_row, n_col),
            out_shape=pltpu.VMEM((nb, yl * zl, n), F32),
            in_specs=[hb] * 5,
            out_specs=vm,
            scratch_shapes=[
                pltpu.VMEM((nb, yl, zl, n), BF16),
                pltpu.VMEM((n, n), BF16),
                pltpu.VMEM((n, n), BF16),
                pltpu.VMEM((n, n), BF16),
                pltpu.VMEM((QUAD * n, QUAD * n), BF16),
                pltpu.VMEM((n, n), BF16),
                pltpu.VMEM((n, n), BF16),
                pltpu.VMEM((CORES * il, jl, n), F32),
                pltpu.VMEM((jl, n, LANES), F32),
                pltpu.VMEM((slabs, TILE * PITCH_Y, LANES), F32),
                pltpu.VMEM((jl * PITCH_Z, LANES), F32),
                pltpu.VMEM((n * PITCH_J, LANES), F32),
                pltpu.VMEM((chunks, n_row, zl, yl, LANES), BF16),
                pltpu.VMEM((chunks, zl, n, LANES), BF16),
                pltpu.VMEM((chunks, n_col, zl, jl, LANES), BF16),
                pltpu.VMEM((chunks, n, jl, LANES), BF16),
                pltpu.VMEM((chunks, n_col, zl, jl, LANES), BF16),
                pltpu.VMEM((chunks, zl, n, LANES), BF16),
                pltpu.VMEM((chunks, n_row, zl, yl, LANES), BF16),
                pltpu.VMEM((chunks, n_row, zl, yl, LANES), BF16),
                dma((tiles,)), dma((3,)), dma, dma, dma,
                dma, dma((units,)), dma, dma((units,)), dma, dma((units,)), dma, dma((units,)),
            ],
            compiler_params=pltpu.CompilerParams(
                collective_id=0, has_side_effects=True, vmem_limit_bytes=50 * 2**20),
            name="pencils",
        )(*(pltpu.with_memory_space_constraint(x, pltpu.HBM) for x in (u, fac_a, fac_b, fac_c, diag_d)))
        w = pl.pallas_call(
            last_kernel,
            out_shape=jax.ShapeDtypeStruct((nb, yl * zl, n), F32),
            in_specs=[vm],
            out_specs=hb,
            scratch_shapes=[dma],
            compiler_params=pltpu.CompilerParams(vmem_limit_bytes=2**20),
            name="last",
        )(pltpu.with_memory_space_constraint(done, pltpu.VMEM)).reshape(nb, yl, zl, n)
        return jnp.transpose(w, (0, 3, 1, 2))

    return jax.shard_map(local_apply, mesh=mesh, in_specs=(spec_field, spec_factor, spec_factor, spec_factor, spec_diag), out_specs=spec_field, check_vma=False)
```

```python
import functools

import jax
import jax.numpy as jnp
from jax import lax
from jax.experimental import pallas as pl
from jax.experimental.pallas import tpu as pltpu
from jax.sharding import PartitionSpec as P

MESH = pl.DeviceIdType.MESH
F32, BF16 = jnp.float32, jnp.bfloat16
CORES = 2
QUAD = 4
TILE = 16
PAIRS = 16
WAIT = 3
SIX = 6
UNIT = 4
LANES = 128
PITCH_Y = 24
PITCH_Z = 136
PITCH_J = 40


def fill_spread(a_ref, w_ref, slabs):
    n = a_ref.shape[0]
    slab = n // slabs
    w_ref[...] = jnp.zeros_like(w_ref)
    for s in range(slabs):
        for b in range(QUAD):
            w_ref[pl.ds(s * n + b * slab, slab), pl.ds(b * n, n)] = a_ref[pl.ds(s * slab, slab), :]


def exchange_kernel(n_row, n_col, u_hbm, a_hbm, b_hbm, c_hbm, d_hbm, w_ref,
                    u_v, a_ref, b_ref, c_ref, w_v, bt_v, ct_v, d_v, dt_v, scr_y, scr_z, scr_j,
                    send_f, recv_f, send_cf, recv_cf, send_cb, recv_cb, send_b, recv_b,
                    u_sem, abc_sem, d_sem, d_send, d_recv, sf, rf, scf, rcf, scb, rcb, sb, rb):
    me = lax.axis_index("row")
    mc = lax.axis_index("col")
    core = lax.rem(me, CORES)
    slabs = n_row // CORES
    n = a_ref.shape[0]
    group = CORES * QUAD
    chunks = u_v.shape[0] // group
    yl, zl = u_v.shape[1], u_v.shape[2]
    jl = n // n_col
    il = d_v.shape[0] // CORES
    tiles = zl // TILE
    per_tile = TILE // UNIT
    per_chunk = zl // UNIT
    units = chunks * per_chunk

    def load_u(q, p):
        sl = (pl.ds(q * group, group), slice(None), pl.ds(p * TILE, TILE))
        return pltpu.make_async_copy(u_hbm.at[sl], u_v.at[sl], u_sem.at[q * tiles + p])

    barrier = pltpu.get_barrier_semaphore()
    for k in range(1, n_row):
        pl.semaphore_signal(barrier, inc=1, device_id={"row": lax.rem(me + k, n_row)}, device_id_type=MESH)
    for k in range(1, n_col):
        pl.semaphore_signal(barrier, inc=1, device_id={"col": lax.rem(mc + k, n_col)}, device_id_type=MESH)

    factors = [pltpu.make_async_copy(x, v, abc_sem.at[k])
               for k, (x, v) in enumerate(((a_hbm, a_ref), (b_hbm, b_ref), (c_hbm, c_ref)))]
    factors[0].start()
    for q in range(chunks):
        for p in range(tiles):
            load_u(q, p).start()
    factors[1].start()
    factors[2].start()
    own_d = pltpu.make_async_copy(d_hbm, d_v.at[pl.ds(core * il, il)], d_sem)
    own_d.start()

    factors[0].wait()
    fill_spread(a_ref, w_v, slabs)

    partner = me + 1 - 2 * core
    pair_d = pltpu.make_async_remote_copy(
        d_hbm, d_v.at[pl.ds(core * il, il)], d_send, d_recv, device_id={"row": partner}, device_id_type=MESH)

    my_y = pl.ds(pl.multiple_of(me * yl, yl), yl)
    my_j = pl.ds(pl.multiple_of(mc * jl, jl), jl)

    row_to = []
    for k in sorted(range(1, slabs), key=lambda k: -min(k, slabs - k)):
        for e in range(CORES):
            row_to.append(lax.rem(me // CORES + k, slabs) * CORES + lax.rem(core + e, CORES))
    row_to += [me - core + lax.rem(core + e, CORES) for e in range(1, CORES)]
    col_to = [lax.rem(mc + k, n_col) for k in sorted(range(1, n_col), key=lambda k: -min(k, n_col - k))]

    def arrived(ref, sem):
        pltpu.make_async_copy(ref, ref, sem).wait()

    def stage_one(v):
        q, p = v // tiles, lax.rem(v, tiles)
        zs = pl.ds(pl.multiple_of(p * TILE, TILE), TILE)
        load_u(q, p).wait()
        for g in range(CORES):
            lhs = jnp.concatenate(
                [u_v[q * group + g * QUAD + b, :, zs, :].reshape(yl * TILE, n) for b in range(QUAD)], axis=1)
            out = lax.dot_general(lhs, w_v[...], (((1,), (1,)), ((), ())), preferred_element_type=F32)
            for s in range(slabs):
                for y in range(yl):
                    scr_y[s, pl.ds(y, TILE, stride=PITCH_Y), :] = out[y * TILE:(y + 1) * TILE, s * LANES:(s + 1) * LANES]
            for s in range(slabs):
                rows = scr_y[s].reshape(TILE, PITCH_Y, LANES)[:, :yl, :]
                send_f[q, s * CORES + g, zs] = rows.astype(BF16)
        recv_f[q, zs, my_y, :] = send_f[q, me, zs]

    def send_one(v):
        q, p = v // tiles, lax.rem(v, tiles)
        for e in range(per_tile):
            part = pl.ds(p * TILE + e * UNIT, UNIT)
            for to in row_to:
                pltpu.make_async_remote_copy(
                    send_f.at[q, to, part], recv_f.at[q, part, my_y, :], sf, rf.at[v * per_tile + e],
                    device_id={"row": to}, device_id_type=MESH).start()

    def stage_two(t):
        q, z0 = t // per_chunk, lax.rem(t, per_chunk) * UNIT
        zs = pl.ds(z0, UNIT)
        arrived(recv_f.at[q, zs, pl.ds(0, n - yl), :], rf.at[t])
        for p in range(0, UNIT, 2):
            rhs = jnp.concatenate([recv_f[q, z0 + p], recv_f[q, z0 + p + 1]], axis=1)
            out = jnp.dot(b_ref[...], rhs, preferred_element_type=F32).astype(BF16)
            for e in range(2):
                for c in range(n_col):
                    send_cf[q, c, z0 + p + e] = out[c * jl:(c + 1) * jl, e * LANES:(e + 1) * LANES]
        land = pl.ds(mc * zl + z0, UNIT)
        recv_cf[q, land] = send_cf[q, mc, zs]
        for to in col_to:
            pltpu.make_async_remote_copy(
                send_cf.at[q, to, zs], recv_cf.at[q, land], scf, rcf.at[t],
                device_id={"col": to}, device_id_type=MESH).start()

    def collect(t):
        q, z0 = t // per_chunk, lax.rem(t, per_chunk) * UNIT
        arrived(recv_cf.at[q, pl.ds(0, (n_col - 1) * UNIT)], rcf.at[t])
        for c in range(n_col):
            for e in range(UNIT):
                z = c * zl + z0 + e
                scr_z[pl.ds(z, jl, stride=PITCH_Z), :] = recv_cf[q, z].astype(F32)

    def stage_mid(q):
        def some(i, _):
            mids = []
            for p in range(PAIRS):
                j = (i * PAIRS + p) * 2
                rhs = jnp.concatenate(
                    [scr_z[pl.ds(pl.multiple_of((j + e) * PITCH_Z, 8), n), :].astype(BF16) for e in range(2)], axis=1)
                mid = jnp.dot(c_ref[...], rhs, preferred_element_type=F32)
                mids.append((mid * jnp.concatenate([dt_v[j], dt_v[j + 1]], axis=1)).astype(BF16))
            for p in range(PAIRS):
                j = (i * PAIRS + p) * 2
                out = jnp.dot(ct_v[...], mids[p], preferred_element_type=F32)
                for e in range(2):
                    scr_j[pl.ds(j + e, n, stride=PITCH_J), :] = out[:, e * LANES:(e + 1) * LANES]
            return 0

        lax.fori_loop(0, jl // (2 * PAIRS), some, 0)
        for c in range(n_col):
            rows = scr_j[pl.ds(c * zl * PITCH_J, zl * PITCH_J), :].reshape(zl, PITCH_J, LANES)[:, :jl, :]
            send_cb[q, c] = rows.astype(BF16)
        recv_cb[q, :, my_j, :] = send_cb[q, mc]

        def send(e, _):
            zs = pl.ds(e * UNIT, UNIT)
            for to in col_to:
                pltpu.make_async_remote_copy(
                    send_cb.at[q, to, zs], recv_cb.at[q, zs, my_j, :], scb, rcb.at[q * per_chunk + e],
                    device_id={"col": to}, device_id_type=MESH).start()
            return 0

        lax.fori_loop(0, per_chunk, send, 0)

    def stage_five(t):
        q, z0 = t // per_chunk, lax.rem(t, per_chunk) * UNIT
        zs = pl.ds(z0, UNIT)
        arrived(recv_cb.at[q, zs, pl.ds(0, n - jl), :], rcb.at[t])
        for p in range(0, UNIT, 2):
            rhs = jnp.concatenate([recv_cb[q, z0 + p], recv_cb[q, z0 + p + 1]], axis=1)
            out = jnp.dot(bt_v[...], rhs, preferred_element_type=F32).astype(BF16)
            for e in range(2):
                for r in range(n_row):
                    send_b[q, r, z0 + p + e] = out[r * yl:(r + 1) * yl, e * LANES:(e + 1) * LANES]
        recv_b[q, me, zs] = send_b[q, me, zs]
        for to in row_to:
            pltpu.make_async_remote_copy(
                send_b.at[q, to, zs], recv_b.at[q, me, zs], sb, rb.at[t], device_id={"row": to}, device_id_type=MESH).start()

    def stage_six(q, z0, planes):
        for e in range(planes // UNIT):
            t = q * per_chunk + z0 // UNIT + e
            arrived(recv_b.at[q, pl.ds(0, n_row - 1), pl.ds(z0 + e * UNIT, UNIT)], rb.at[t])
        for g in range(CORES):
            lhs = jnp.concatenate(
                [recv_b[q, s * CORES + g, pl.ds(z0, planes)].reshape(planes * yl, LANES) for s in range(slabs)], axis=1)
            out = jnp.dot(lhs, w_v[...], preferred_element_type=F32)
            for b in range(QUAD):
                for e in range(planes):
                    w_ref[q * group + g * QUAD + b, pl.ds(z0 + e, yl, stride=PITCH_J), :] = (
                        out[e * yl:(e + 1) * yl, b * LANES:(b + 1) * LANES])

    def build_d(t):
        for e in range(jl // per_chunk):
            j = t * (jl // per_chunk) + e
            rows = d_v[:, pl.ds(j, 1), :].reshape(CORES * il, n)
            dt_v[j] = jnp.concatenate([rows] * QUAD, axis=0).T

    stage_one(0)
    pl.semaphore_wait(barrier, n_row + n_col - 2)
    send_one(0)
    pair_d.start()
    stage_one(1)
    send_one(1)
    factors[1].wait()
    factors[2].wait()
    bt_v[...] = b_ref[...].astype(F32).T.astype(BF16)
    ct_v[...] = c_ref[...].astype(F32).T.astype(BF16)
    own_d.wait()
    pair_d.wait()
    lead = 2
    lag = per_chunk
    after = lag + per_chunk + WAIT

    def tick(t, _):
        @pl.when(t < units)
        def _():
            stage_two(t)

        @pl.when((lax.rem(t, per_tile) == 0) & (t // per_tile + lead < chunks * tiles))
        def _():
            stage_one(t // per_tile + lead)
            send_one(t // per_tile + lead)

        @pl.when(t < per_chunk)
        def _():
            build_d(t)

        @pl.when((t >= lag) & (t < units + lag))
        def _():
            collect(t - lag)

            @pl.when(lax.rem(t - lag, per_chunk) == per_chunk - 1)
            def _():
                stage_mid((t - lag) // per_chunk)

        @pl.when((t >= after) & (t < units + after))
        def _():
            stage_five(t - after)

        done = t - after - SIX

        @pl.when((done >= 0) & (done < units - per_tile) & (lax.rem(done, per_tile) == per_tile - 1))
        def _():
            v = done // per_tile
            stage_six(v // tiles, lax.rem(v, tiles) * TILE, TILE)

        return 0

    lax.fori_loop(0, units + after, tick, 0)
    for v in range((units + after - SIX - after) // per_tile, chunks * tiles - 1):
        stage_six(v // tiles, v % tiles * TILE, TILE)
    for e in range(per_tile):
        stage_six(chunks - 1, (tiles - 1) * TILE + e * UNIT, UNIT)

    arrived(send_f.at[:, pl.ds(0, n_row - 1)], sf)
    arrived(send_cf.at[:, pl.ds(0, n_col - 1)], scf)
    arrived(send_cb.at[:, pl.ds(0, n_col - 1)], scb)
    arrived(send_b.at[:, pl.ds(0, n_row - 1)], sb)


def last_kernel(w_ref, w_hbm, sem):
    nb, yl, zl, n = w_hbm.shape
    pieces = 8
    for i in range(pieces):
        part = pl.ds(i * (nb // pieces), nb // pieces)
        pltpu.make_async_copy(w_ref.at[part, :, pl.ds(0, zl)], w_hbm.at[part], sem).start()
    pltpu.make_async_copy(w_hbm, w_hbm, sem).wait()


def solution(mesh):
    spec_field = P("fields", None, "row", "col")
    spec_factor = P("fields", None)
    spec_diag = P(("fields", "row"), "col", None)
    n_row, n_col = mesh.shape["row"], mesh.shape["col"]
    slabs = n_row // CORES

    def local_apply(field_u, fac_a, fac_b, fac_c, diag_d):
        nb, n, yl, zl = field_u.shape
        il, jl, _ = diag_d.shape
        chunks = nb // (CORES * QUAD)
        tiles = chunks * zl // TILE
        units = chunks * zl // UNIT
        u = jnp.transpose(field_u, (0, 2, 3, 1))
        vm = pl.BlockSpec(memory_space=pltpu.VMEM)
        hb = pl.BlockSpec(memory_space=pltpu.HBM)
        dma = pltpu.SemaphoreType.DMA
        done = pl.pallas_call(
            functools.partial(exchange_kernel, n_row, n_col),
            out_shape=pltpu.VMEM((nb, yl * PITCH_J, n), F32),
            in_specs=[hb] * 5,
            out_specs=vm,
            scratch_shapes=[
                pltpu.VMEM((nb, yl, zl, n), BF16),
                pltpu.VMEM((n, n), BF16),
                pltpu.VMEM((n, n), BF16),
                pltpu.VMEM((n, n), BF16),
                pltpu.VMEM((QUAD * n, QUAD * n), BF16),
                pltpu.VMEM((n, n), BF16),
                pltpu.VMEM((n, n), BF16),
                pltpu.VMEM((CORES * il, jl, n), F32),
                pltpu.VMEM((jl, n, LANES), F32),
                pltpu.VMEM((slabs, TILE * PITCH_Y, LANES), F32),
                pltpu.VMEM((jl * PITCH_Z, LANES), F32),
                pltpu.VMEM((n * PITCH_J, LANES), F32),
                pltpu.VMEM((chunks, n_row, zl, yl, LANES), BF16),
                pltpu.VMEM((chunks, zl, n, LANES), BF16),
                pltpu.VMEM((chunks, n_col, zl, jl, LANES), BF16),
                pltpu.VMEM((chunks, n, jl, LANES), BF16),
                pltpu.VMEM((chunks, n_col, zl, jl, LANES), BF16),
                pltpu.VMEM((chunks, zl, n, LANES), BF16),
                pltpu.VMEM((chunks, n_row, zl, yl, LANES), BF16),
                pltpu.VMEM((chunks, n_row, zl, yl, LANES), BF16),
                dma((tiles,)), dma((3,)), dma, dma, dma,
                dma, dma((units,)), dma, dma((units,)), dma, dma((units,)), dma, dma((units,)),
            ],
            compiler_params=pltpu.CompilerParams(
                collective_id=0, has_side_effects=True, vmem_limit_bytes=48 * 2**20),
            name="pencils",
        )(*(pltpu.with_memory_space_constraint(x, pltpu.HBM) for x in (u, fac_a, fac_b, fac_c, diag_d)))
        w = pl.pallas_call(
            last_kernel,
            out_shape=jax.ShapeDtypeStruct((nb, yl, zl, n), F32),
            in_specs=[vm],
            out_specs=hb,
            scratch_shapes=[dma],
            compiler_params=pltpu.CompilerParams(vmem_limit_bytes=2**20),
            name="last",
        )(pltpu.with_memory_space_constraint(done.reshape(nb, yl, PITCH_J, n), pltpu.VMEM))
        return jnp.transpose(w, (0, 3, 1, 2))

    return jax.shard_map(local_apply, mesh=mesh, in_specs=(spec_field, spec_factor, spec_factor, spec_factor, spec_diag), out_specs=spec_field, check_vma=False)
```

```python
import functools

import jax
import jax.numpy as jnp
from jax import lax
from jax.experimental import pallas as pl
from jax.experimental.pallas import tpu as pltpu
from jax.sharding import PartitionSpec as P

MESH = pl.DeviceIdType.MESH
F32, BF16 = jnp.float32, jnp.bfloat16
CORES = 2
QUAD = 4
TILE = 16
PAIRS = 16
WAIT = 3
SIX = 6
UNIT = 4
LANES = 128
PITCH_Y = 24
PITCH_Z = 136
PITCH_J = 40


def fill_spread(a_ref, w_ref, slabs):
    n = a_ref.shape[0]
    slab = n // slabs
    w_ref[...] = jnp.zeros_like(w_ref)
    for s in range(slabs):
        for b in range(QUAD):
            w_ref[pl.ds(s * n + b * slab, slab), pl.ds(b * n, n)] = a_ref[pl.ds(s * slab, slab), :]


def exchange_kernel(n_row, n_col, u_hbm, a_hbm, b_hbm, c_hbm, d_hbm, w_ref,
                    u_v, a_ref, b_ref, c_ref, w_v, bt_v, ct_v, d_v, dt_v, scr_y, scr_z, scr_j,
                    send_f, recv_f, send_cf, recv_cf, send_cb, recv_cb, send_b, recv_b,
                    u_sem, abc_sem, d_sem, d_send, d_recv, sf, rf, scf, rcf, scb, rcb, sb, rb):
    me = lax.axis_index("row")
    mc = lax.axis_index("col")
    core = lax.rem(me, CORES)
    slabs = n_row // CORES
    n = a_ref.shape[0]
    group = CORES * QUAD
    chunks = u_v.shape[0] // group
    yl, zl = u_v.shape[1], u_v.shape[2]
    jl = n // n_col
    il = d_v.shape[0] // CORES
    tiles = zl // TILE
    per_tile = TILE // UNIT
    per_chunk = zl // UNIT
    units = chunks * per_chunk

    def load_u(q, p):
        sl = (pl.ds(q * group, group), slice(None), pl.ds(p * TILE, TILE))
        return pltpu.make_async_copy(u_hbm.at[sl], u_v.at[sl], u_sem.at[q * tiles + p])

    barrier = pltpu.get_barrier_semaphore()
    for k in range(1, n_row):
        pl.semaphore_signal(barrier, inc=1, device_id={"row": lax.rem(me + k, n_row)}, device_id_type=MESH)
    for k in range(1, n_col):
        pl.semaphore_signal(barrier, inc=1, device_id={"col": lax.rem(mc + k, n_col)}, device_id_type=MESH)

    factors = [pltpu.make_async_copy(x, v, abc_sem.at[k])
               for k, (x, v) in enumerate(((a_hbm, a_ref), (b_hbm, b_ref), (c_hbm, c_ref)))]
    factors[0].start()
    for q in range(chunks):
        for p in range(tiles):
            load_u(q, p).start()
    factors[1].start()
    factors[2].start()
    own_d = pltpu.make_async_copy(d_hbm, d_v.at[pl.ds(core * il, il)], d_sem)
    own_d.start()

    factors[0].wait()
    fill_spread(a_ref, w_v, slabs)

    partner = me + 1 - 2 * core
    pair_d = pltpu.make_async_remote_copy(
        d_hbm, d_v.at[pl.ds(core * il, il)], d_send, d_recv, device_id={"row": partner}, device_id_type=MESH)

    my_y = pl.ds(pl.multiple_of(me * yl, yl), yl)
    my_j = pl.ds(pl.multiple_of(mc * jl, jl), jl)

    row_to = []
    for k in sorted(range(1, slabs), key=lambda k: -min(k, slabs - k)):
        for e in range(CORES):
            row_to.append(lax.rem(me // CORES + k, slabs) * CORES + lax.rem(core + e, CORES))
    row_to += [me - core + lax.rem(core + e, CORES) for e in range(1, CORES)]
    col_to = [lax.rem(mc + k, n_col) for k in sorted(range(1, n_col), key=lambda k: -min(k, n_col - k))]

    def arrived(ref, sem):
        pltpu.make_async_copy(ref, ref, sem).wait()

    def stage_one(v):
        q, p = v // tiles, lax.rem(v, tiles)
        zs = pl.ds(pl.multiple_of(p * TILE, TILE), TILE)
        load_u(q, p).wait()
        for g in range(CORES):
            lhs = jnp.concatenate(
                [u_v[q * group + g * QUAD + b, :, zs, :].reshape(yl * TILE, n) for b in range(QUAD)], axis=1)
            out = lax.dot_general(lhs, w_v[...], (((1,), (1,)), ((), ())), preferred_element_type=F32)
            for s in range(slabs):
                for y in range(yl):
                    scr_y[s, pl.ds(y, TILE, stride=PITCH_Y), :] = out[y * TILE:(y + 1) * TILE, s * LANES:(s + 1) * LANES]
            for s in range(slabs):
                rows = scr_y[s].reshape(TILE, PITCH_Y, LANES)[:, :yl, :]
                send_f[q, s * CORES + g, zs] = rows.astype(BF16)
        recv_f[q, zs, my_y, :] = send_f[q, me, zs]

    def send_one(v):
        q, p = v // tiles, lax.rem(v, tiles)
        for e in range(per_tile):
            part = pl.ds(p * TILE + e * UNIT, UNIT)
            for to in row_to:
                pltpu.make_async_remote_copy(
                    send_f.at[q, to, part], recv_f.at[q, part, my_y, :], sf, rf.at[v * per_tile + e],
                    device_id={"row": to}, device_id_type=MESH).start()

    def stage_two(t):
        q, z0 = t // per_chunk, lax.rem(t, per_chunk) * UNIT
        zs = pl.ds(z0, UNIT)
        arrived(recv_f.at[q, zs, pl.ds(0, n - yl), :], rf.at[t])
        for p in range(0, UNIT, 2):
            rhs = jnp.concatenate([recv_f[q, z0 + p], recv_f[q, z0 + p + 1]], axis=1)
            out = jnp.dot(b_ref[...], rhs, preferred_element_type=F32).astype(BF16)
            for e in range(2):
                for c in range(n_col):
                    send_cf[q, c, z0 + p + e] = out[c * jl:(c + 1) * jl, e * LANES:(e + 1) * LANES]
        land = pl.ds(mc * zl + z0, UNIT)
        for to in col_to:
            pltpu.make_async_remote_copy(
                send_cf.at[q, to, zs], recv_cf.at[q, land], scf, rcf.at[t],
                device_id={"col": to}, device_id_type=MESH).start()
        recv_cf[q, land] = send_cf[q, mc, zs]

    def collect(t):
        q, z0 = t // per_chunk, lax.rem(t, per_chunk) * UNIT
        arrived(recv_cf.at[q, pl.ds(0, (n_col - 1) * UNIT)], rcf.at[t])
        for c in range(n_col):
            for e in range(UNIT):
                z = c * zl + z0 + e
                scr_z[pl.ds(z, jl, stride=PITCH_Z), :] = recv_cf[q, z].astype(F32)

    def stage_mid(q):
        def some(i, _):
            mids = []
            for p in range(PAIRS):
                j = (i * PAIRS + p) * 2
                rhs = jnp.concatenate(
                    [scr_z[pl.ds(pl.multiple_of((j + e) * PITCH_Z, 8), n), :].astype(BF16) for e in range(2)], axis=1)
                mid = jnp.dot(c_ref[...], rhs, preferred_element_type=F32)
                mids.append((mid * jnp.concatenate([dt_v[j], dt_v[j + 1]], axis=1)).astype(BF16))
            for p in range(PAIRS):
                j = (i * PAIRS + p) * 2
                out = jnp.dot(ct_v[...], mids[p], preferred_element_type=F32)
                for e in range(2):
                    scr_j[pl.ds(j + e, n, stride=PITCH_J), :] = out[:, e * LANES:(e + 1) * LANES]
            return 0

        lax.fori_loop(0, jl // (2 * PAIRS), some, 0)

        def send(e, _):
            zs = pl.ds(e * UNIT, UNIT)
            for c in range(n_col):
                first = pl.multiple_of((c * zl + e * UNIT) * PITCH_J, 8)
                rows = scr_j[pl.ds(first, UNIT * PITCH_J), :].reshape(UNIT, PITCH_J, LANES)[:, :jl, :]
                send_cb[q, c, zs] = rows.astype(BF16)
            for to in col_to:
                pltpu.make_async_remote_copy(
                    send_cb.at[q, to, zs], recv_cb.at[q, zs, my_j, :], scb, rcb.at[q * per_chunk + e],
                    device_id={"col": to}, device_id_type=MESH).start()
            return 0

        lax.fori_loop(0, per_chunk, send, 0)
        recv_cb[q, :, my_j, :] = send_cb[q, mc]

    def stage_five(t):
        q, z0 = t // per_chunk, lax.rem(t, per_chunk) * UNIT
        zs = pl.ds(z0, UNIT)
        arrived(recv_cb.at[q, zs, pl.ds(0, n - jl), :], rcb.at[t])
        for p in range(0, UNIT, 2):
            rhs = jnp.concatenate([recv_cb[q, z0 + p], recv_cb[q, z0 + p + 1]], axis=1)
            out = jnp.dot(bt_v[...], rhs, preferred_element_type=F32).astype(BF16)
            for e in range(2):
                for r in range(n_row):
                    send_b[q, r, z0 + p + e] = out[r * yl:(r + 1) * yl, e * LANES:(e + 1) * LANES]
        for to in row_to:
            pltpu.make_async_remote_copy(
                send_b.at[q, to, zs], recv_b.at[q, me, zs], sb, rb.at[t], device_id={"row": to}, device_id_type=MESH).start()

        recv_b[q, me, zs] = send_b[q, me, zs]

    def stage_six(q, z0, planes):
        for e in range(planes // UNIT):
            t = q * per_chunk + z0 // UNIT + e
            arrived(recv_b.at[q, pl.ds(0, n_row - 1), pl.ds(z0 + e * UNIT, UNIT)], rb.at[t])
        for g in range(CORES):
            lhs = jnp.concatenate(
                [recv_b[q, s * CORES + g, pl.ds(z0, planes)].reshape(planes * yl, LANES) for s in range(slabs)], axis=1)
            out = jnp.dot(lhs, w_v[...], preferred_element_type=F32)
            for b in range(QUAD):
                for e in range(planes):
                    w_ref[q * group + g * QUAD + b, pl.ds(z0 + e, yl, stride=PITCH_J), :] = (
                        out[e * yl:(e + 1) * yl, b * LANES:(b + 1) * LANES])

    def build_d(t):
        for e in range(jl // per_chunk):
            j = t * (jl // per_chunk) + e
            rows = d_v[:, pl.ds(j, 1), :].reshape(CORES * il, n)
            dt_v[j] = jnp.concatenate([rows] * QUAD, axis=0).T

    stage_one(0)
    pl.semaphore_wait(barrier, n_row + n_col - 2)
    send_one(0)
    pair_d.start()
    stage_one(1)
    send_one(1)
    factors[1].wait()
    factors[2].wait()
    bt_v[...] = b_ref[...].astype(F32).T.astype(BF16)
    ct_v[...] = c_ref[...].astype(F32).T.astype(BF16)
    own_d.wait()
    pair_d.wait()
    lead = 2
    lag = per_chunk
    after = lag + per_chunk + WAIT

    def tick(t, _):
        @pl.when(t < units)
        def _():
            stage_two(t)

        @pl.when((lax.rem(t, per_tile) == 0) & (t // per_tile + lead < chunks * tiles))
        def _():
            stage_one(t // per_tile + lead)
            send_one(t // per_tile + lead)

        @pl.when(t < per_chunk)
        def _():
            build_d(t)

        @pl.when((t >= lag) & (t < units + lag))
        def _():
            collect(t - lag)

            @pl.when(lax.rem(t - lag, per_chunk) == per_chunk - 1)
            def _():
                stage_mid((t - lag) // per_chunk)

        @pl.when((t >= after) & (t < units + after))
        def _():
            stage_five(t - after)

        done = t - after - SIX

        @pl.when((done >= 0) & (done < units - per_tile) & (lax.rem(done, per_tile) == per_tile - 1))
        def _():
            v = done // per_tile
            stage_six(v // tiles, lax.rem(v, tiles) * TILE, TILE)

        return 0

    lax.fori_loop(0, units + after, tick, 0)
    for v in range((units + after - SIX - after) // per_tile, chunks * tiles - 1):
        stage_six(v // tiles, v % tiles * TILE, TILE)
    for e in range(per_tile):
        stage_six(chunks - 1, (tiles - 1) * TILE + e * UNIT, UNIT)

    arrived(send_f.at[:, pl.ds(0, n_row - 1)], sf)
    arrived(send_cf.at[:, pl.ds(0, n_col - 1)], scf)
    arrived(send_cb.at[:, pl.ds(0, n_col - 1)], scb)
    arrived(send_b.at[:, pl.ds(0, n_row - 1)], sb)


def last_kernel(w_ref, w_hbm, sem):
    nb, yl, zl, n = w_hbm.shape
    pieces = 32
    for i in range(pieces):
        part = pl.ds(i * (nb // pieces), nb // pieces)
        pltpu.make_async_copy(w_ref.at[part, :, pl.ds(0, zl)], w_hbm.at[part], sem).start()
    pltpu.make_async_copy(w_hbm, w_hbm, sem).wait()


def solution(mesh):
    spec_field = P("fields", None, "row", "col")
    spec_factor = P("fields", None)
    spec_diag = P(("fields", "row"), "col", None)
    n_row, n_col = mesh.shape["row"], mesh.shape["col"]
    slabs = n_row // CORES

    def local_apply(field_u, fac_a, fac_b, fac_c, diag_d):
        nb, n, yl, zl = field_u.shape
        il, jl, _ = diag_d.shape
        chunks = nb // (CORES * QUAD)
        tiles = chunks * zl // TILE
        units = chunks * zl // UNIT
        u = jnp.transpose(field_u, (0, 2, 3, 1))
        vm = pl.BlockSpec(memory_space=pltpu.VMEM)
        hb = pl.BlockSpec(memory_space=pltpu.HBM)
        dma = pltpu.SemaphoreType.DMA
        done = pl.pallas_call(
            functools.partial(exchange_kernel, n_row, n_col),
            out_shape=pltpu.VMEM((nb, yl * PITCH_J, n), F32),
            in_specs=[hb] * 5,
            out_specs=vm,
            scratch_shapes=[
                pltpu.VMEM((nb, yl, zl, n), BF16),
                pltpu.VMEM((n, n), BF16),
                pltpu.VMEM((n, n), BF16),
                pltpu.VMEM((n, n), BF16),
                pltpu.VMEM((QUAD * n, QUAD * n), BF16),
                pltpu.VMEM((n, n), BF16),
                pltpu.VMEM((n, n), BF16),
                pltpu.VMEM((CORES * il, jl, n), F32),
                pltpu.VMEM((jl, n, LANES), F32),
                pltpu.VMEM((slabs, TILE * PITCH_Y, LANES), F32),
                pltpu.VMEM((jl * PITCH_Z, LANES), F32),
                pltpu.VMEM((n * PITCH_J, LANES), F32),
                pltpu.VMEM((chunks, n_row, zl, yl, LANES), BF16),
                pltpu.VMEM((chunks, zl, n, LANES), BF16),
                pltpu.VMEM((chunks, n_col, zl, jl, LANES), BF16),
                pltpu.VMEM((chunks, n, jl, LANES), BF16),
                pltpu.VMEM((chunks, n_col, zl, jl, LANES), BF16),
                pltpu.VMEM((chunks, zl, n, LANES), BF16),
                pltpu.VMEM((chunks, n_row, zl, yl, LANES), BF16),
                pltpu.VMEM((chunks, n_row, zl, yl, LANES), BF16),
                dma((tiles,)), dma((3,)), dma, dma, dma,
                dma, dma((units,)), dma, dma((units,)), dma, dma((units,)), dma, dma((units,)),
            ],
            compiler_params=pltpu.CompilerParams(
                collective_id=0, has_side_effects=True, vmem_limit_bytes=48 * 2**20),
            name="pencils",
        )(*(pltpu.with_memory_space_constraint(x, pltpu.HBM) for x in (u, fac_a, fac_b, fac_c, diag_d)))
        w = pl.pallas_call(
            last_kernel,
            out_shape=jax.ShapeDtypeStruct((nb, yl, zl, n), F32),
            in_specs=[vm],
            out_specs=hb,
            scratch_shapes=[dma],
            compiler_params=pltpu.CompilerParams(vmem_limit_bytes=2**20),
            name="last",
        )(pltpu.with_memory_space_constraint(done.reshape(nb, yl, PITCH_J, n), pltpu.VMEM))
        return jnp.transpose(w, (0, 3, 1, 2))

    return jax.shard_map(local_apply, mesh=mesh, in_specs=(spec_field, spec_factor, spec_factor, spec_factor, spec_diag), out_specs=spec_field, check_vma=False)
```

```python
import functools

import jax
import jax.numpy as jnp
from jax import lax
from jax.experimental import pallas as pl
from jax.experimental.pallas import tpu as pltpu
from jax.sharding import PartitionSpec as P

MESH = pl.DeviceIdType.MESH
F32, BF16 = jnp.float32, jnp.bfloat16
CORES = 2
QUAD = 4
TILE = 16
PAIRS = 16
WAIT = 3
SIX = 6
UNIT = 4
LANES = 128
PITCH_Y = 24
PITCH_Z = 136
PITCH_J = 40


def fill_spread(a_ref, w_ref, slabs):
    n = a_ref.shape[0]
    slab = n // slabs
    w_ref[...] = jnp.zeros_like(w_ref)
    for s in range(slabs):
        for b in range(QUAD):
            w_ref[pl.ds(s * n + b * slab, slab), pl.ds(b * n, n)] = a_ref[pl.ds(s * slab, slab), :]


def exchange_kernel(n_row, n_col, u_hbm, a_hbm, b_hbm, c_hbm, d_hbm, w_ref,
                    u_v, a_ref, b_ref, c_ref, w_v, bt_v, ct_v, d_v, dt_v, scr_y, scr_z, scr_j,
                    send_f, recv_f, send_cf, recv_cf, send_cb, recv_cb, send_b, recv_b,
                    u_sem, abc_sem, d_sem, d_send, d_recv, sf, rf, scf, rcf, scb, rcb, sb, rb):
    me = lax.axis_index("row")
    mc = lax.axis_index("col")
    core = lax.rem(me, CORES)
    slabs = n_row // CORES
    n = a_ref.shape[0]
    group = CORES * QUAD
    chunks = u_v.shape[0] // group
    yl, zl = u_v.shape[1], u_v.shape[2]
    jl = n // n_col
    il = d_v.shape[0] // CORES
    tiles = zl // TILE
    per_tile = TILE // UNIT
    per_chunk = zl // UNIT
    units = chunks * per_chunk

    def load_u(q, p):
        sl = (pl.ds(q * group, group), slice(None), pl.ds(p * TILE, TILE))
        return pltpu.make_async_copy(u_hbm.at[sl], u_v.at[sl], u_sem.at[q * tiles + p])

    barrier = pltpu.get_barrier_semaphore()
    for k in range(1, n_row):
        pl.semaphore_signal(barrier, inc=1, device_id={"row": lax.rem(me + k, n_row)}, device_id_type=MESH)
    for k in range(1, n_col):
        pl.semaphore_signal(barrier, inc=1, device_id={"col": lax.rem(mc + k, n_col)}, device_id_type=MESH)

    factors = [pltpu.make_async_copy(x, v, abc_sem.at[k])
               for k, (x, v) in enumerate(((a_hbm, a_ref), (b_hbm, b_ref), (c_hbm, c_ref)))]
    factors[0].start()
    for q in range(chunks):
        for p in range(tiles):
            load_u(q, p).start()
    factors[1].start()
    factors[2].start()
    own_d = pltpu.make_async_copy(d_hbm, d_v.at[pl.ds(core * il, il)], d_sem)
    own_d.start()

    factors[0].wait()
    fill_spread(a_ref, w_v, slabs)

    partner = me + 1 - 2 * core
    pair_d = pltpu.make_async_remote_copy(
        d_hbm, d_v.at[pl.ds(core * il, il)], d_send, d_recv, device_id={"row": partner}, device_id_type=MESH)

    my_y = pl.ds(pl.multiple_of(me * yl, yl), yl)
    my_j = pl.ds(pl.multiple_of(mc * jl, jl), jl)

    row_to = []
    for k in sorted(range(1, slabs), key=lambda k: -min(k, slabs - k)):
        for e in range(CORES):
            row_to.append(lax.rem(me // CORES + k, slabs) * CORES + lax.rem(core + e, CORES))
    row_to += [me - core + lax.rem(core + e, CORES) for e in range(1, CORES)]
    col_to = [lax.rem(mc + k, n_col) for k in sorted(range(1, n_col), key=lambda k: -min(k, n_col - k))]

    def arrived(ref, sem):
        pltpu.make_async_copy(ref, ref, sem).wait()

    def stage_one(v):
        q, p = v // tiles, lax.rem(v, tiles)
        zs = pl.ds(pl.multiple_of(p * TILE, TILE), TILE)
        load_u(q, p).wait()
        for g in range(CORES):
            lhs = jnp.concatenate(
                [u_v[q * group + g * QUAD + b, :, zs, :].reshape(yl * TILE, n) for b in range(QUAD)], axis=1)
            out = lax.dot_general(lhs, w_v[...], (((1,), (1,)), ((), ())), preferred_element_type=F32)
            for s in range(slabs):
                for y in range(yl):
                    scr_y[s, pl.ds(y, TILE, stride=PITCH_Y), :] = out[y * TILE:(y + 1) * TILE, s * LANES:(s + 1) * LANES]
            for s in range(slabs):
                rows = scr_y[s].reshape(TILE, PITCH_Y, LANES)[:, :yl, :]
                send_f[q, s * CORES + g, zs] = rows.astype(BF16)
        recv_f[q, zs, my_y, :] = send_f[q, me, zs]

    def send_one(v):
        q, p = v // tiles, lax.rem(v, tiles)
        for e in range(per_tile):
            part = pl.ds(p * TILE + e * UNIT, UNIT)
            for to in row_to:
                pltpu.make_async_remote_copy(
                    send_f.at[q, to, part], recv_f.at[q, part, my_y, :], sf, rf.at[v * per_tile + e],
                    device_id={"row": to}, device_id_type=MESH).start()

    def stage_two(t):
        q, z0 = t // per_chunk, lax.rem(t, per_chunk) * UNIT
        zs = pl.ds(z0, UNIT)
        arrived(recv_f.at[q, zs, pl.ds(0, n - yl), :], rf.at[t])
        for p in range(0, UNIT, 2):
            rhs = jnp.concatenate([recv_f[q, z0 + p], recv_f[q, z0 + p + 1]], axis=1)
            out = jnp.dot(b_ref[...], rhs, preferred_element_type=F32).astype(BF16)
            for e in range(2):
                for c in range(n_col):
                    send_cf[q, c, z0 + p + e] = out[c * jl:(c + 1) * jl, e * LANES:(e + 1) * LANES]
        land = pl.ds(mc * zl + z0, UNIT)
        for to in col_to:
            pltpu.make_async_remote_copy(
                send_cf.at[q, to, zs], recv_cf.at[q, land], scf, rcf.at[t],
                device_id={"col": to}, device_id_type=MESH).start()
        recv_cf[q, land] = send_cf[q, mc, zs]

    def collect(t):
        q, z0 = t // per_chunk, lax.rem(t, per_chunk) * UNIT
        arrived(recv_cf.at[q, pl.ds(0, (n_col - 1) * UNIT)], rcf.at[t])
        for c in range(n_col):
            for e in range(UNIT):
                z = c * zl + z0 + e
                scr_z[pl.ds(z, jl, stride=PITCH_Z), :] = recv_cf[q, z].astype(F32)

    def stage_mid(q):
        def some(i, _):
            mids = []
            for p in range(PAIRS):
                j = (i * PAIRS + p) * 2
                rhs = jnp.concatenate(
                    [scr_z[pl.ds(pl.multiple_of((j + e) * PITCH_Z, 8), n), :].astype(BF16) for e in range(2)], axis=1)
                mid = jnp.dot(c_ref[...], rhs, preferred_element_type=F32)
                mids.append((mid * jnp.concatenate([dt_v[j], dt_v[j + 1]], axis=1)).astype(BF16))
            for p in range(PAIRS):
                j = (i * PAIRS + p) * 2
                out = jnp.dot(ct_v[...], mids[p], preferred_element_type=F32)
                for e in range(2):
                    scr_j[pl.ds(j + e, n, stride=PITCH_J), :] = out[:, e * LANES:(e + 1) * LANES]
            return 0

        lax.fori_loop(0, jl // (2 * PAIRS), some, 0)

        def send(e, _):
            zs = pl.ds(e * UNIT, UNIT)
            for c in range(n_col):
                first = pl.multiple_of((c * zl + e * UNIT) * PITCH_J, 8)
                rows = scr_j[pl.ds(first, UNIT * PITCH_J), :].reshape(UNIT, PITCH_J, LANES)[:, :jl, :]
                send_cb[q, c, zs] = rows.astype(BF16)
            for to in col_to:
                pltpu.make_async_remote_copy(
                    send_cb.at[q, to, zs], recv_cb.at[q, zs, my_j, :], scb, rcb.at[q * per_chunk + e],
                    device_id={"col": to}, device_id_type=MESH).start()
            return 0

        lax.fori_loop(0, per_chunk, send, 0)
        recv_cb[q, :, my_j, :] = send_cb[q, mc]

    def stage_five(t):
        q, z0 = t // per_chunk, lax.rem(t, per_chunk) * UNIT
        zs = pl.ds(z0, UNIT)
        arrived(recv_cb.at[q, zs, pl.ds(0, n - jl), :], rcb.at[t])
        for p in range(0, UNIT, 2):
            rhs = jnp.concatenate([recv_cb[q, z0 + p], recv_cb[q, z0 + p + 1]], axis=1)
            out = jnp.dot(bt_v[...], rhs, preferred_element_type=F32).astype(BF16)
            for e in range(2):
                for r in range(n_row):
                    send_b[q, r, z0 + p + e] = out[r * yl:(r + 1) * yl, e * LANES:(e + 1) * LANES]
        for to in row_to:
            pltpu.make_async_remote_copy(
                send_b.at[q, to, zs], recv_b.at[q, me, zs], sb, rb.at[t], device_id={"row": to}, device_id_type=MESH).start()

        recv_b[q, me, zs] = send_b[q, me, zs]

    def stage_six(q, z0, planes):
        for e in range(planes // UNIT):
            t = q * per_chunk + z0 // UNIT + e
            arrived(recv_b.at[q, pl.ds(0, n_row - 1), pl.ds(z0 + e * UNIT, UNIT)], rb.at[t])
        rows = planes * yl
        lhs = jnp.concatenate([
            jnp.concatenate(
                [recv_b[q, s * CORES + g, pl.ds(z0, planes)].reshape(rows, LANES) for s in range(slabs)], axis=1)
            for g in range(CORES)], axis=0)
        out = jnp.dot(lhs, w_v[...], preferred_element_type=F32)
        for g in range(CORES):
            for b in range(QUAD):
                for e in range(planes):
                    w_ref[q * group + g * QUAD + b, pl.ds(z0 + e, yl, stride=PITCH_J), :] = (
                        out[g * rows + e * yl:g * rows + (e + 1) * yl, b * LANES:(b + 1) * LANES])

    def build_d(t):
        for e in range(jl // per_chunk):
            j = t * (jl // per_chunk) + e
            rows = d_v[:, pl.ds(j, 1), :].reshape(CORES * il, n)
            dt_v[j] = jnp.concatenate([rows] * QUAD, axis=0).T

    stage_one(0)
    pl.semaphore_wait(barrier, n_row + n_col - 2)
    send_one(0)
    pair_d.start()
    stage_one(1)
    send_one(1)
    factors[1].wait()
    factors[2].wait()
    bt_v[...] = b_ref[...].astype(F32).T.astype(BF16)
    ct_v[...] = c_ref[...].astype(F32).T.astype(BF16)
    own_d.wait()
    pair_d.wait()
    lead = 2
    lag = per_chunk
    after = lag + per_chunk + WAIT

    def tick(t, _):
        @pl.when(t < units)
        def _():
            stage_two(t)

        @pl.when((lax.rem(t, per_tile) == 0) & (t // per_tile + lead < chunks * tiles))
        def _():
            stage_one(t // per_tile + lead)
            send_one(t // per_tile + lead)

        @pl.when(t < per_chunk)
        def _():
            build_d(t)

        @pl.when((t >= lag) & (t < units + lag))
        def _():
            collect(t - lag)

            @pl.when(lax.rem(t - lag, per_chunk) == per_chunk - 1)
            def _():
                stage_mid((t - lag) // per_chunk)

        @pl.when((t >= after) & (t < units + after))
        def _():
            stage_five(t - after)

        done = t - after - SIX

        @pl.when((done >= 0) & (done < units - per_tile) & (lax.rem(done, per_tile) == per_tile - 1))
        def _():
            v = done // per_tile
            stage_six(v // tiles, lax.rem(v, tiles) * TILE, TILE)

        return 0

    lax.fori_loop(0, units + after, tick, 0)
    for v in range((units + after - SIX - after) // per_tile, chunks * tiles - 1):
        stage_six(v // tiles, v % tiles * TILE, TILE)
    for e in range(per_tile):
        stage_six(chunks - 1, (tiles - 1) * TILE + e * UNIT, UNIT)

    arrived(send_f.at[:, pl.ds(0, n_row - 1)], sf)
    arrived(send_cf.at[:, pl.ds(0, n_col - 1)], scf)
    arrived(send_cb.at[:, pl.ds(0, n_col - 1)], scb)
    arrived(send_b.at[:, pl.ds(0, n_row - 1)], sb)


def last_kernel(w_ref, w_hbm, sem):
    nb, yl, zl, n = w_hbm.shape
    pieces = 32
    for i in range(pieces):
        part = pl.ds(i * (nb // pieces), nb // pieces)
        pltpu.make_async_copy(w_ref.at[part, :, pl.ds(0, zl)], w_hbm.at[part], sem).start()
    pltpu.make_async_copy(w_hbm, w_hbm, sem).wait()


def solution(mesh):
    spec_field = P("fields", None, "row", "col")
    spec_factor = P("fields", None)
    spec_diag = P(("fields", "row"), "col", None)
    n_row, n_col = mesh.shape["row"], mesh.shape["col"]
    slabs = n_row // CORES

    def local_apply(field_u, fac_a, fac_b, fac_c, diag_d):
        nb, n, yl, zl = field_u.shape
        il, jl, _ = diag_d.shape
        chunks = nb // (CORES * QUAD)
        tiles = chunks * zl // TILE
        units = chunks * zl // UNIT
        u = jnp.transpose(field_u, (0, 2, 3, 1))
        vm = pl.BlockSpec(memory_space=pltpu.VMEM)
        hb = pl.BlockSpec(memory_space=pltpu.HBM)
        dma = pltpu.SemaphoreType.DMA
        done = pl.pallas_call(
            functools.partial(exchange_kernel, n_row, n_col),
            out_shape=pltpu.VMEM((nb, yl * PITCH_J, n), F32),
            in_specs=[hb] * 5,
            out_specs=vm,
            scratch_shapes=[
                pltpu.VMEM((nb, yl, zl, n), BF16),
                pltpu.VMEM((n, n), BF16),
                pltpu.VMEM((n, n), BF16),
                pltpu.VMEM((n, n), BF16),
                pltpu.VMEM((QUAD * n, QUAD * n), BF16),
                pltpu.VMEM((n, n), BF16),
                pltpu.VMEM((n, n), BF16),
                pltpu.VMEM((CORES * il, jl, n), F32),
                pltpu.VMEM((jl, n, LANES), F32),
                pltpu.VMEM((slabs, TILE * PITCH_Y, LANES), F32),
                pltpu.VMEM((jl * PITCH_Z, LANES), F32),
                pltpu.VMEM((n * PITCH_J, LANES), F32),
                pltpu.VMEM((chunks, n_row, zl, yl, LANES), BF16),
                pltpu.VMEM((chunks, zl, n, LANES), BF16),
                pltpu.VMEM((chunks, n_col, zl, jl, LANES), BF16),
                pltpu.VMEM((chunks, n, jl, LANES), BF16),
                pltpu.VMEM((chunks, n_col, zl, jl, LANES), BF16),
                pltpu.VMEM((chunks, zl, n, LANES), BF16),
                pltpu.VMEM((chunks, n_row, zl, yl, LANES), BF16),
                pltpu.VMEM((chunks, n_row, zl, yl, LANES), BF16),
                dma((tiles,)), dma((3,)), dma, dma, dma,
                dma, dma((units,)), dma, dma((units,)), dma, dma((units,)), dma, dma((units,)),
            ],
            compiler_params=pltpu.CompilerParams(
                collective_id=0, has_side_effects=True, vmem_limit_bytes=48 * 2**20),
            name="pencils",
        )(*(pltpu.with_memory_space_constraint(x, pltpu.HBM) for x in (u, fac_a, fac_b, fac_c, diag_d)))
        w = pl.pallas_call(
            last_kernel,
            out_shape=jax.ShapeDtypeStruct((nb, yl, zl, n), F32),
            in_specs=[vm],
            out_specs=hb,
            scratch_shapes=[dma],
            compiler_params=pltpu.CompilerParams(vmem_limit_bytes=2**20),
            name="last",
        )(pltpu.with_memory_space_constraint(done.reshape(nb, yl, PITCH_J, n), pltpu.VMEM))
        return jnp.transpose(w, (0, 3, 1, 2))

    return jax.shard_map(local_apply, mesh=mesh, in_specs=(spec_field, spec_factor, spec_factor, spec_factor, spec_diag), out_specs=spec_field, check_vma=False)
```

```python
import functools

import jax
import jax.numpy as jnp
from jax import lax
from jax.experimental import pallas as pl
from jax.experimental.pallas import tpu as pltpu
from jax.sharding import PartitionSpec as P

MESH = pl.DeviceIdType.MESH
F32, BF16 = jnp.float32, jnp.bfloat16
CORES = 2
QUAD = 4
TILE = 16
PAIRS = 16
WAIT = 3
SIX = 6
UNIT = 4
LANES = 128
PITCH_Y = 24
PITCH_Z = 136
PITCH_J = 40


def fill_spread(a_ref, w_ref, slabs):
    n = a_ref.shape[0]
    slab = n // slabs
    w_ref[...] = jnp.zeros_like(w_ref)
    for s in range(slabs):
        for b in range(QUAD):
            w_ref[pl.ds(s * n + b * slab, slab), pl.ds(b * n, n)] = a_ref[pl.ds(s * slab, slab), :]


def exchange_kernel(n_row, n_col, u_hbm, a_hbm, b_hbm, c_hbm, d_hbm, w_ref,
                    u_v, a_ref, b_ref, c_ref, w_v, bt_v, ct_v, d_v, dt_v, scr_y, scr_z, scr_j,
                    send_f, recv_f, send_cf, recv_cf, send_cb, recv_cb, send_b, recv_b,
                    u_sem, abc_sem, d_sem, d_send, d_recv, sf, rf, scf, rcf, scb, rcb, sb, rb):
    me = lax.axis_index("row")
    mc = lax.axis_index("col")
    core = lax.rem(me, CORES)
    slabs = n_row // CORES
    n = a_ref.shape[0]
    group = CORES * QUAD
    chunks = u_v.shape[0] // group
    yl, zl = u_v.shape[1], u_v.shape[2]
    jl = n // n_col
    il = d_v.shape[0] // CORES
    tiles = zl // TILE
    per_tile = TILE // UNIT
    per_chunk = zl // UNIT
    units = chunks * per_chunk

    def load_u(q, p):
        sl = (pl.ds(q * group, group), slice(None), pl.ds(p * TILE, TILE))
        return pltpu.make_async_copy(u_hbm.at[sl], u_v.at[sl], u_sem.at[q * tiles + p])

    barrier = pltpu.get_barrier_semaphore()
    for k in range(1, n_row):
        pl.semaphore_signal(barrier, inc=1, device_id={"row": lax.rem(me + k, n_row)}, device_id_type=MESH)
    for k in range(1, n_col):
        pl.semaphore_signal(barrier, inc=1, device_id={"col": lax.rem(mc + k, n_col)}, device_id_type=MESH)

    factors = [pltpu.make_async_copy(x, v, abc_sem.at[k])
               for k, (x, v) in enumerate(((a_hbm, a_ref), (b_hbm, b_ref), (c_hbm, c_ref)))]
    factors[0].start()
    for q in range(chunks):
        for p in range(tiles):
            load_u(q, p).start()
    factors[1].start()
    factors[2].start()
    own_d = pltpu.make_async_copy(d_hbm, d_v.at[pl.ds(core * il, il)], d_sem)
    own_d.start()

    factors[0].wait()
    fill_spread(a_ref, w_v, slabs)

    partner = me + 1 - 2 * core
    pair_d = pltpu.make_async_remote_copy(
        d_hbm, d_v.at[pl.ds(core * il, il)], d_send, d_recv, device_id={"row": partner}, device_id_type=MESH)

    my_y = pl.ds(pl.multiple_of(me * yl, yl), yl)
    my_j = pl.ds(pl.multiple_of(mc * jl, jl), jl)

    row_to = []
    for k in sorted(range(1, slabs), key=lambda k: -min(k, slabs - k)):
        for e in range(CORES):
            row_to.append(lax.rem(me // CORES + k, slabs) * CORES + lax.rem(core + e, CORES))
    row_to += [me - core + lax.rem(core + e, CORES) for e in range(1, CORES)]
    col_to = [lax.rem(mc + k, n_col) for k in sorted(range(1, n_col), key=lambda k: -min(k, n_col - k))]

    def arrived(ref, sem):
        pltpu.make_async_copy(ref, ref, sem).wait()

    def stage_one(v):
        q, p = v // tiles, lax.rem(v, tiles)
        zs = pl.ds(pl.multiple_of(p * TILE, TILE), TILE)
        load_u(q, p).wait()
        for g in range(CORES):
            lhs = jnp.concatenate(
                [u_v[q * group + g * QUAD + b, :, zs, :].reshape(yl * TILE, n) for b in range(QUAD)], axis=1)
            out = lax.dot_general(lhs, w_v[...], (((1,), (1,)), ((), ())), preferred_element_type=F32)
            for s in range(slabs):
                for y in range(yl):
                    scr_y[s, pl.ds(y, TILE, stride=PITCH_Y), :] = out[y * TILE:(y + 1) * TILE, s * LANES:(s + 1) * LANES]
            for s in range(slabs):
                rows = scr_y[s].reshape(TILE, PITCH_Y, LANES)[:, :yl, :]
                send_f[q, s * CORES + g, zs] = rows.astype(BF16)
        recv_f[q, zs, my_y, :] = send_f[q, me, zs]

    def send_one(v):
        q, p = v // tiles, lax.rem(v, tiles)
        for e in range(per_tile):
            part = pl.ds(p * TILE + e * UNIT, UNIT)
            for to in row_to:
                pltpu.make_async_remote_copy(
                    send_f.at[q, to, part], recv_f.at[q, part, my_y, :], sf, rf.at[v * per_tile + e],
                    device_id={"row": to}, device_id_type=MESH).start()

    def stage_two(t):
        q, z0 = t // per_chunk, lax.rem(t, per_chunk) * UNIT
        zs = pl.ds(z0, UNIT)
        arrived(recv_f.at[q, zs, pl.ds(0, n - yl), :], rf.at[t])
        for p in range(0, UNIT, 2):
            rhs = jnp.concatenate([recv_f[q, z0 + p], recv_f[q, z0 + p + 1]], axis=1)
            out = jnp.dot(b_ref[...], rhs, preferred_element_type=F32).astype(BF16)
            for e in range(2):
                for c in range(n_col):
                    send_cf[q, c, z0 + p + e] = out[c * jl:(c + 1) * jl, e * LANES:(e + 1) * LANES]
        land = pl.ds(mc * zl + z0, UNIT)
        for to in col_to:
            pltpu.make_async_remote_copy(
                send_cf.at[q, to, zs], recv_cf.at[q, land], scf, rcf.at[t],
                device_id={"col": to}, device_id_type=MESH).start()
        recv_cf[q, land] = send_cf[q, mc, zs]

    def collect(t):
        q, z0 = t // per_chunk, lax.rem(t, per_chunk) * UNIT
        arrived(recv_cf.at[q, pl.ds(0, (n_col - 1) * UNIT)], rcf.at[t])
        for c in range(n_col):
            for e in range(UNIT):
                z = c * zl + z0 + e
                scr_z[pl.ds(z, jl, stride=PITCH_Z), :] = recv_cf[q, z].astype(F32)

    def stage_mid(q):
        def some(i, _):
            mids = []
            for p in range(PAIRS):
                j = (i * PAIRS + p) * 2
                rhs = jnp.concatenate(
                    [scr_z[pl.ds(pl.multiple_of((j + e) * PITCH_Z, 8), n), :].astype(BF16) for e in range(2)], axis=1)
                mid = jnp.dot(c_ref[...], rhs, preferred_element_type=F32)
                mids.append((mid * jnp.concatenate([dt_v[j], dt_v[j + 1]], axis=1)).astype(BF16))
            for p in range(PAIRS):
                j = (i * PAIRS + p) * 2
                out = jnp.dot(ct_v[...], mids[p], preferred_element_type=F32)
                for e in range(2):
                    scr_j[pl.ds(j + e, n, stride=PITCH_J), :] = out[:, e * LANES:(e + 1) * LANES]
            return 0

        lax.fori_loop(0, jl // (2 * PAIRS), some, 0)

        def send(e, _):
            zs = pl.ds(e * UNIT, UNIT)
            for c in range(n_col):
                first = pl.multiple_of((c * zl + e * UNIT) * PITCH_J, 8)
                rows = scr_j[pl.ds(first, UNIT * PITCH_J), :].reshape(UNIT, PITCH_J, LANES)[:, :jl, :]
                send_cb[q, c, zs] = rows.astype(BF16)
            for to in col_to:
                pltpu.make_async_remote_copy(
                    send_cb.at[q, to, zs], recv_cb.at[q, zs, my_j, :], scb, rcb.at[q * per_chunk + e],
                    device_id={"col": to}, device_id_type=MESH).start()
            return 0

        lax.fori_loop(0, per_chunk, send, 0)
        recv_cb[q, :, my_j, :] = send_cb[q, mc]

    def stage_five(t):
        q, z0 = t // per_chunk, lax.rem(t, per_chunk) * UNIT
        zs = pl.ds(z0, UNIT)
        arrived(recv_cb.at[q, zs, pl.ds(0, n - jl), :], rcb.at[t])
        for p in range(0, UNIT, 2):
            rhs = jnp.concatenate([recv_cb[q, z0 + p], recv_cb[q, z0 + p + 1]], axis=1)
            out = jnp.dot(bt_v[...], rhs, preferred_element_type=F32).astype(BF16)
            for e in range(2):
                for r in range(n_row):
                    send_b[q, r, z0 + p + e] = out[r * yl:(r + 1) * yl, e * LANES:(e + 1) * LANES]
        for to in row_to:
            pltpu.make_async_remote_copy(
                send_b.at[q, to, zs], recv_b.at[q, me, zs], sb, rb.at[t], device_id={"row": to}, device_id_type=MESH).start()

        recv_b[q, me, zs] = send_b[q, me, zs]

    def stage_six(q, z0, planes):
        for e in range(planes // UNIT):
            t = q * per_chunk + z0 // UNIT + e
            arrived(recv_b.at[q, pl.ds(0, n_row - 1), pl.ds(z0 + e * UNIT, UNIT)], rb.at[t])
        rows = planes * yl
        lhs = jnp.concatenate([
            jnp.concatenate(
                [recv_b[q, s * CORES + g, pl.ds(z0, planes)].reshape(rows, LANES) for s in range(slabs)], axis=1)
            for g in range(CORES)], axis=0)
        out = jnp.dot(lhs, w_v[...], preferred_element_type=F32)
        for g in range(CORES):
            for b in range(QUAD):
                for e in range(planes):
                    w_ref[q * group + g * QUAD + b, pl.ds(z0 + e, yl, stride=PITCH_J), :] = (
                        out[g * rows + e * yl:g * rows + (e + 1) * yl, b * LANES:(b + 1) * LANES])

    def build_d(t):
        for e in range(jl // per_chunk):
            j = t * (jl // per_chunk) + e
            rows = d_v[:, pl.ds(j, 1), :].reshape(CORES * il, n)
            dt_v[j] = jnp.concatenate([rows] * QUAD, axis=0).T

    stage_one(0)
    pl.semaphore_wait(barrier, n_row + n_col - 2)
    send_one(0)
    pair_d.start()
    stage_one(1)
    send_one(1)
    factors[1].wait()
    factors[2].wait()
    bt_v[...] = b_ref[...].astype(F32).T.astype(BF16)
    ct_v[...] = c_ref[...].astype(F32).T.astype(BF16)
    own_d.wait()
    pair_d.wait()
    lead = 2
    lag = per_chunk
    after = lag + per_chunk + WAIT

    def tick(t, _):
        @pl.when(t < units)
        def _():
            stage_two(t)

        @pl.when((lax.rem(t, per_tile) == 0) & (t // per_tile + lead < chunks * tiles))
        def _():
            stage_one(t // per_tile + lead)
            send_one(t // per_tile + lead)

        @pl.when(t < per_chunk)
        def _():
            build_d(t)

        @pl.when((t >= lag) & (t < units + lag))
        def _():
            collect(t - lag)

            @pl.when(lax.rem(t - lag, per_chunk) == per_chunk - 1)
            def _():
                stage_mid((t - lag) // per_chunk)

        @pl.when((t >= after) & (t < units + after))
        def _():
            stage_five(t - after)

        done = t - after - SIX

        @pl.when((done >= 0) & (done < units - per_tile) & (lax.rem(done, per_tile) == per_tile - 1))
        def _():
            v = done // per_tile
            stage_six(v // tiles, lax.rem(v, tiles) * TILE, TILE)

        return 0

    lax.fori_loop(0, units + after, tick, 0)
    for v in range((units + after - SIX - after) // per_tile, chunks * tiles - 1):
        stage_six(v // tiles, v % tiles * TILE, TILE)
    for e in range(per_tile):
        stage_six(chunks - 1, (tiles - 1) * TILE + e * UNIT, UNIT)

    arrived(send_f.at[:, pl.ds(0, n_row - 1)], sf)
    arrived(send_cf.at[:, pl.ds(0, n_col - 1)], scf)
    arrived(send_cb.at[:, pl.ds(0, n_col - 1)], scb)
    arrived(send_b.at[:, pl.ds(0, n_row - 1)], sb)


def last_kernel(w_ref, w_hbm, sem):
    nb, yl, zl, n = w_hbm.shape
    for i in range(nb):
        for half in (pl.ds(0, yl // 2), pl.ds(yl // 2, yl // 2)):
            pltpu.make_async_copy(w_ref.at[i, half, pl.ds(0, zl)], w_hbm.at[i, half], sem).start()
    pltpu.make_async_copy(w_hbm, w_hbm, sem).wait()


def solution(mesh):
    spec_field = P("fields", None, "row", "col")
    spec_factor = P("fields", None)
    spec_diag = P(("fields", "row"), "col", None)
    n_row, n_col = mesh.shape["row"], mesh.shape["col"]
    slabs = n_row // CORES

    def local_apply(field_u, fac_a, fac_b, fac_c, diag_d):
        nb, n, yl, zl = field_u.shape
        il, jl, _ = diag_d.shape
        chunks = nb // (CORES * QUAD)
        tiles = chunks * zl // TILE
        units = chunks * zl // UNIT
        u = jnp.transpose(field_u, (0, 2, 3, 1))
        vm = pl.BlockSpec(memory_space=pltpu.VMEM)
        hb = pl.BlockSpec(memory_space=pltpu.HBM)
        dma = pltpu.SemaphoreType.DMA
        done = pl.pallas_call(
            functools.partial(exchange_kernel, n_row, n_col),
            out_shape=pltpu.VMEM((nb, yl * PITCH_J, n), F32),
            in_specs=[hb] * 5,
            out_specs=vm,
            scratch_shapes=[
                pltpu.VMEM((nb, yl, zl, n), BF16),
                pltpu.VMEM((n, n), BF16),
                pltpu.VMEM((n, n), BF16),
                pltpu.VMEM((n, n), BF16),
                pltpu.VMEM((QUAD * n, QUAD * n), BF16),
                pltpu.VMEM((n, n), BF16),
                pltpu.VMEM((n, n), BF16),
                pltpu.VMEM((CORES * il, jl, n), F32),
                pltpu.VMEM((jl, n, LANES), F32),
                pltpu.VMEM((slabs, TILE * PITCH_Y, LANES), F32),
                pltpu.VMEM((jl * PITCH_Z, LANES), F32),
                pltpu.VMEM((n * PITCH_J, LANES), F32),
                pltpu.VMEM((chunks, n_row, zl, yl, LANES), BF16),
                pltpu.VMEM((chunks, zl, n, LANES), BF16),
                pltpu.VMEM((chunks, n_col, zl, jl, LANES), BF16),
                pltpu.VMEM((chunks, n, jl, LANES), BF16),
                pltpu.VMEM((chunks, n_col, zl, jl, LANES), BF16),
                pltpu.VMEM((chunks, zl, n, LANES), BF16),
                pltpu.VMEM((chunks, n_row, zl, yl, LANES), BF16),
                pltpu.VMEM((chunks, n_row, zl, yl, LANES), BF16),
                dma((tiles,)), dma((3,)), dma, dma, dma,
                dma, dma((units,)), dma, dma((units,)), dma, dma((units,)), dma, dma((units,)),
            ],
            compiler_params=pltpu.CompilerParams(
                collective_id=0, has_side_effects=True, vmem_limit_bytes=48 * 2**20),
            name="pencils",
        )(*(pltpu.with_memory_space_constraint(x, pltpu.HBM) for x in (u, fac_a, fac_b, fac_c, diag_d)))
        w = pl.pallas_call(
            last_kernel,
            out_shape=jax.ShapeDtypeStruct((nb, yl, zl, n), F32),
            in_specs=[vm],
            out_specs=hb,
            scratch_shapes=[dma],
            compiler_params=pltpu.CompilerParams(vmem_limit_bytes=2**20),
            name="last",
        )(pltpu.with_memory_space_constraint(done.reshape(nb, yl, PITCH_J, n), pltpu.VMEM))
        return jnp.transpose(w, (0, 3, 1, 2))

    return jax.shard_map(local_apply, mesh=mesh, in_specs=(spec_field, spec_factor, spec_factor, spec_factor, spec_diag), out_specs=spec_field, check_vma=False)
```
